32 devices in a mesh: freq: 16 (over z, x, core), grid: 2 (over y).
Axes of the slice: x: 2, y: 2, z: 4, core: 2. Of those that a mesh axis runs over, the one named last changes fastest.
Arguments:
- cross_spectra: float32 [2, 32, 256, 256], P(None, None, 'freq', 'grid'), as said below
- sensor_modes: float32 [32, 96, 256], P('freq', None, 'grid'), may hold values from -0.375 to 0.375
- source_modes: float32 [32, 96, 256], P('freq', None, 'grid'), may hold values from -6 to 6
- wavenumber: float32 [32, 96], P('freq'), may hold values from 0.5 to 2
- attenuation: float32 [32, 96], P('freq'), may hold values from 0.002 to 0.03
- mode_counts: int32 [32], P('freq'), may hold values from 48 to 96
Outputs:
- bartlett_power: float32 [64, 256], P('freq', 'grid')
The draws below stay inside these ranges and needn't reach their ends.
Inputs may be any that keep to these rules, and one draw needn't show every extreme that they name: `cross_spectra`: each bin's matrix K_f is Hermitian and positive definite. Modes with index mode_counts[f] or more are left out in bin f.
All inputs are finite; a program needn't handle non-finite values.
Results may differ from the reference program's by a relative error of at most 0.0003.
Values sent between devices are 32-bit elements; how exact they have to be, the bound alone decides.
A program may use at most 128 MiB of HBM per device.

```python
import math
import jax
import jax.numpy as jnp
from jax import lax

SENSORS = 256
MODES = 96
RANGES = 64
BINS = 32
DEPTHS = 256


def sensor_table(key):
    base = jax.random.fold_in(key, 201)
    values = jnp.clip(jax.random.normal(base, (BINS, MODES, SENSORS), jnp.float32), -6.0, 6.0)
    return (values / math.sqrt(SENSORS)).astype(jnp.float32)


def source_table(key):
    base = jax.random.fold_in(key, 202)
    values = jnp.clip(jax.random.normal(base, (BINS, MODES, DEPTHS), jnp.float32), -6.0, 6.0)
    return values.astype(jnp.float32)


def wave_table(key):
    base = jax.random.fold_in(key, 203)
    values = jnp.exp(jax.random.uniform(base, (BINS, MODES), jnp.float32, math.log(0.5), math.log(2.0)))
    return jnp.clip(values, 0.5, 2.0).astype(jnp.float32)


def atten_table(key):
    base = jax.random.fold_in(key, 204)
    values = jnp.exp(jax.random.uniform(base, (BINS, MODES), jnp.float32, math.log(0.002), math.log(0.03)))
    return jnp.clip(values, 0.002, 0.03).astype(jnp.float32)


def draw_sensor_modes(key, part):
    return sensor_table(key)


def draw_source_modes(key, part):
    return source_table(key)


def draw_wavenumber(key, part):
    return wave_table(key)


def draw_attenuation(key, part):
    return atten_table(key)


def draw_cross_spectra(key, part):
    snapshots = SENSORS // 2
    planted = 3
    key_real, key_imag, key_gain, key_bin, key_range, key_depth, key_power = jax.random.split(jax.random.fold_in(key, 17), 7)
    sample_real = jax.random.normal(key_real, (BINS, SENSORS, snapshots), jnp.float32) * math.sqrt(0.5)
    sample_imag = jax.random.normal(key_imag, (BINS, SENSORS, snapshots), jnp.float32) * math.sqrt(0.5)
    sensor_gain = jnp.exp(jax.random.uniform(key_gain, (BINS, SENSORS), jnp.float32, math.log(0.5), math.log(2.0)))
    bin_gain = jnp.exp(jax.random.uniform(key_bin, (BINS,), jnp.float32, math.log(0.3), math.log(3.0)))
    noise_real = (jnp.einsum('bis,bjs->bij', sample_real, sample_real) + jnp.einsum('bis,bjs->bij', sample_imag, sample_imag)) / snapshots
    noise_real = noise_real + jnp.eye(SENSORS, dtype=jnp.float32)[None]
    noise_imag = (jnp.einsum('bis,bjs->bij', sample_imag, sample_real) - jnp.einsum('bis,bjs->bij', sample_real, sample_imag)) / snapshots
    gain_outer = sensor_gain[:, :, None] * sensor_gain[:, None, :]
    noise_real = noise_real * gain_outer
    noise_imag = noise_imag * gain_outer
    shapes = sensor_table(key)
    sources = source_table(key)
    waves = wave_table(key)
    damping = atten_table(key)
    cell_range = jax.random.randint(key_range, (planted,), 0, RANGES)
    cell_depth = jax.random.randint(key_depth, (planted,), 0, DEPTHS)
    radius = 1.0 + cell_range.astype(jnp.float32)
    phase = waves[:, :, None] * radius[None, None, :]
    magnitude = jnp.exp(-damping[:, :, None] * radius[None, None, :]) / jnp.sqrt(phase)
    depth_shape = jnp.take(sources, cell_depth, axis=2)
    coef_real = magnitude * jnp.cos(phase) * depth_shape
    coef_imag = magnitude * jnp.sin(phase) * depth_shape
    steer_real = jnp.einsum('bmi,bmp->bpi', shapes, coef_real)
    steer_imag = jnp.einsum('bmi,bmp->bpi', shapes, coef_imag)
    length = jnp.sqrt(jnp.sum(steer_real * steer_real + steer_imag * steer_imag, axis=2, keepdims=True))
    unit_real = steer_real / length
    unit_imag = steer_imag / length
    noise_level = 2.0 * jnp.mean(sensor_gain * sensor_gain, axis=1)
    strength = jnp.exp(jax.random.uniform(key_power, (BINS, planted), jnp.float32, 0.0, math.log(10.0))) * noise_level[:, None]
    signal_real = jnp.einsum('bp,bpi,bpj->bij', strength, unit_real, unit_real) + jnp.einsum('bp,bpi,bpj->bij', strength, unit_imag, unit_imag)
    signal_imag = jnp.einsum('bp,bpi,bpj->bij', strength, unit_imag, unit_real) - jnp.einsum('bp,bpi,bpj->bij', strength, unit_real, unit_imag)
    real_part = (noise_real + signal_real) * bin_gain[:, None, None]
    imag_part = (noise_imag + signal_imag) * bin_gain[:, None, None]
    return jnp.stack([real_part, imag_part]).astype(jnp.float32)


def set_ends(result, stream_key, smallest, high):
    extent = result.shape
    index_at = [jax.random.randint(jax.random.fold_in(stream_key, axis), (), 0, extent[axis]) for axis in range(len(extent))]
    result = result.at[tuple(index_at)].set(smallest)
    longest = extent.index(max(extent))
    index_at[longest] = (index_at[longest] + 1) % extent[longest]
    return result.at[tuple(index_at)].set(high)


def setup_inputs(seed: int = 0) -> dict:
    keys = jax.random.split(jax.random.key(seed), 7)
    cross_spectra = draw_cross_spectra(jax.random.fold_in(keys[6], 71), 0)
    sensor_modes = draw_sensor_modes(jax.random.fold_in(keys[6], 71), 0)
    source_modes = draw_source_modes(jax.random.fold_in(keys[6], 71), 0)
    wavenumber = draw_wavenumber(jax.random.fold_in(keys[6], 71), 0)
    attenuation = draw_attenuation(jax.random.fold_in(keys[6], 71), 0)
    mode_counts = set_ends(jax.random.randint(keys[5], (BINS,), MODES // 2, MODES + 1), jax.random.fold_in(keys[5], 1), MODES // 2, MODES).astype(jnp.int32)
    return dict(cross_spectra=cross_spectra, sensor_modes=sensor_modes, source_modes=source_modes, wavenumber=wavenumber, attenuation=attenuation, mode_counts=mode_counts)


HIGH = lax.Precision.HIGHEST

def replica_terms(wave_row, atten_row, count, source_row, ranges):
    phase = wave_row[:, None] * ranges[None, :]
    magnitude = jnp.exp(-atten_row[:, None] * ranges[None, :]) / jnp.sqrt(phase)
    keep = (jnp.arange(source_row.shape[0], dtype=jnp.int32) < count).astype(jnp.float32)
    hankel_real = magnitude * jnp.cos(phase) * keep[:, None]
    hankel_imag = magnitude * jnp.sin(phase) * keep[:, None]
    coef_real = hankel_real[:, :, None] * source_row[:, None, :]
    coef_imag = hankel_imag[:, :, None] * source_row[:, None, :]
    return (coef_real, coef_imag)

def reference(cross_spectra, sensor_modes, source_modes, wavenumber, attenuation, mode_counts):
    ranges = 1.0 + jnp.arange(RANGES, dtype=jnp.float32)

    def one_bin(total, bin_index):
        spectra = cross_spectra[:, bin_index]
        shapes = sensor_modes[bin_index]
        product = jnp.einsum('cij,mj->cim', spectra, shapes, precision=HIGH)
        projected = jnp.einsum('mi,cin->cmn', shapes, product, precision=HIGH)
        gram = jnp.einsum('mi,ni->mn', shapes, shapes, precision=HIGH)
        coef_real, coef_imag = replica_terms(wavenumber[bin_index], attenuation[bin_index], mode_counts[bin_index], source_modes[bin_index], ranges)
        image_real = jnp.einsum('mn,nrz->mrz', projected[0], coef_real, precision=HIGH) - jnp.einsum('mn,nrz->mrz', projected[1], coef_imag, precision=HIGH)
        image_imag = jnp.einsum('mn,nrz->mrz', projected[1], coef_real, precision=HIGH) + jnp.einsum('mn,nrz->mrz', projected[0], coef_imag, precision=HIGH)
        numer = lax.optimization_barrier(jnp.sum(coef_real * image_real + coef_imag * image_imag, axis=0))
        gram_real = jnp.einsum('mn,nrz->mrz', gram, coef_real, precision=HIGH)
        gram_imag = jnp.einsum('mn,nrz->mrz', gram, coef_imag, precision=HIGH)
        denom = lax.optimization_barrier(jnp.sum(coef_real * gram_real + coef_imag * gram_imag, axis=0))
        return (total + numer / denom, None)
    total, unused = lax.scan(one_bin, jnp.zeros((RANGES, DEPTHS), jnp.float32), jnp.arange(BINS, dtype=jnp.int32))
    return total / BINS
```

```python
import functools

import jax
import jax.numpy as jnp
from jax import lax
from jax.experimental import pallas as pl
from jax.experimental.pallas import tpu as pltpu
from jax.sharding import PartitionSpec as P

RANGES = 64
BLOCK = 8
LANES = 128

HIGH = lax.Precision.HIGHEST
MESH = pl.DeviceIdType.MESH
NT = (((1,), (1,)), ((), ()))


def kernel(
    nf, ng,
    spectra_hbm, sensor_hbm, source_hbm, wave_ref, atten_ref, counts_ref,
    out_ref,
    raw, outgoing, table, shapes, sources, shapes_wide, halves, weight, rows_scr, cols_scr, row_in,
    u_scr, v_scr, lhs, denom, power, parts,
    raw_sem, own_sem, mode_send, mode_recv, send_sem, recv_sem, part_send, part_recv,
):
    devices = nf * ng
    bins = outgoing.shape[0]
    nb = bins // devices
    row_count, col_count = raw.shape[2], raw.shape[3]
    modes = shapes.shape[2]
    ranges = u_scr.shape[1]
    share = ranges // nf
    depth_here = sources.shape[3]
    my_f, my_g = lax.axis_index("freq"), lax.axis_index("grid")
    me = my_f * ng + my_g

    raw_copy = pltpu.make_async_copy(spectra_hbm, raw, raw_sem)
    raw_copy.start()
    own = pl.ds(my_g * nb, nb)
    own_shapes = pltpu.make_async_copy(sensor_hbm.at[own], shapes.at[my_g], own_sem.at[0])
    own_sources = pltpu.make_async_copy(source_hbm.at[own], sources.at[my_g], own_sem.at[1])
    own_shapes.start()
    own_sources.start()

    barrier = pltpu.get_barrier_semaphore()

    def greet(k, carry):
        peer = lax.rem(me + k, devices)
        pl.semaphore_signal(
            barrier, inc=1, device_id=(peer // ng, lax.rem(peer, ng)), device_id_type=MESH
        )
        return carry

    lax.fori_loop(1, devices, greet, 0)

    raw_copy.wait()
    outgoing[...] = raw[0] + raw[1]
    my_rows = pl.ds(pl.multiple_of(my_f * row_count, row_count), row_count)
    for b in range(nb):
        table[my_g, b, my_rows, :] = outgoing[me * nb + b]

    pl.semaphore_wait(barrier, devices - 1)

    def mode_copies(k):
        peer = lax.rem(my_g + k, ng)
        theirs = pl.ds(peer * nb, nb)
        return [
            pltpu.make_async_remote_copy(
                src_ref=hbm.at[theirs],
                dst_ref=here.at[my_g],
                send_sem=mode_send.at[i, k],
                recv_sem=mode_recv.at[i, k],
                device_id=(my_f, peer),
                device_id_type=MESH,
            )
            for i, (hbm, here) in enumerate(((sensor_hbm, shapes), (source_hbm, sources)))
        ]

    for k in range(1, ng):
        for copy in mode_copies(k):
            copy.start()

    def piece(k):
        peer = lax.rem(me + k, devices)
        return pltpu.make_async_remote_copy(
            src_ref=outgoing.at[pl.ds(peer * nb, nb)],
            dst_ref=table.at[my_g, :, my_rows, :],
            send_sem=send_sem.at[k],
            recv_sem=recv_sem.at[k],
            device_id=(peer // ng, lax.rem(peer, ng)),
            device_id_type=MESH,
        )

    def send_piece(k, carry):
        piece(k).start()
        return carry

    lax.fori_loop(1, devices, send_piece, 0)

    for b in range(nb):
        row = my_g * nb + b
        row_in[...] = jnp.ones_like(row_in)
        row_in[0:1, 0:modes] = wave_ref[pl.ds(row, 1), :]
        row_in[1:2, 0:modes] = atten_ref[pl.ds(row, 1), :]
        radius = 1.0 + lax.broadcasted_iota(jnp.int32, (ranges, LANES), 0).astype(jnp.float32)
        lane = lax.broadcasted_iota(jnp.int32, (ranges, LANES), 1)
        phase = radius * row_in[0:1, :]
        magnitude = jnp.exp(-row_in[1:2, :] * radius) / jnp.sqrt(phase)
        magnitude = jnp.where(lane < counts_ref[row], magnitude, 0.0)
        filler = jnp.zeros((LANES - ranges, LANES), jnp.float32)
        for i, factor in enumerate((magnitude * jnp.cos(phase), magnitude * jnp.sin(phase))):
            rows_scr[b, i] = factor
            turned = jnp.concatenate([factor, filler], 0).T
            for blk in range(ranges // BLOCK):
                cols_scr[b, i, blk] = turned[0:modes, blk * BLOCK : (blk + 1) * BLOCK]

    own_shapes.wait()
    own_sources.wait()
    for k in range(1, ng):
        for copy in mode_copies(k):
            copy.wait_recv()

    shapes_wide[...] = jnp.zeros_like(shapes_wide)
    halves[...] = jnp.zeros_like(halves)
    for b in range(nb):
        for g in range(ng):
            shapes_wide[b, 0:modes, g * col_count : (g + 1) * col_count] = shapes[g, b]
            exact = sources[g, b]
            rounded = exact.astype(jnp.bfloat16)
            at = slice(g * depth_here, (g + 1) * depth_here)
            halves[b, 0:modes, at] = rounded
            halves[b, LANES : LANES + modes, at] = rounded
            weight[b, :, at] = 2.0 * exact - rounded.astype(jnp.float32)

    def put(k, block):
        high = block.astype(jnp.bfloat16)
        low = (block - high.astype(jnp.float32)).astype(jnp.bfloat16)
        lhs[k * modes : (k + 1) * modes, 0:LANES] = high
        lhs[k * modes : (k + 1) * modes, LANES : 2 * LANES] = low

    def forms(b):
        image = jnp.dot(lhs[...], halves[b], preferred_element_type=jnp.float32)
        image = image.reshape(BLOCK, modes, image.shape[1]) * weight[b][None]
        return jnp.sum(image, axis=1)

    for b in range(nb):
        wide = shapes_wide[b]
        gram = lax.dot_general(
            wide[0:modes], wide, NT, precision=HIGH, preferred_element_type=jnp.float32
        )

        def denom_block(blk, carry):
            first = pl.multiple_of(blk * BLOCK, BLOCK)
            row_real = rows_scr[b, 0, pl.ds(first, BLOCK), :]
            row_imag = rows_scr[b, 1, pl.ds(first, BLOCK), :]
            col_real, col_imag = cols_scr[b, 0, blk], cols_scr[b, 1, blk]
            for k in range(BLOCK):
                nr, ni = row_real[k : k + 1, :], row_imag[k : k + 1, :]
                mr = jnp.broadcast_to(col_real[:, k : k + 1], (modes, LANES))
                mi = jnp.broadcast_to(col_imag[:, k : k + 1], (modes, LANES))
                u = mr * nr + mi * ni
                u_scr[b, first + k] = u
                v_scr[b, first + k] = mr * ni - mi * nr
                put(k, gram * u)
            denom[b, pl.ds(first, BLOCK), :] = forms(b)
            return carry

        lax.fori_loop(0, ranges // BLOCK, denom_block, 0)

    def take_piece(k, carry):
        piece(k).wait_recv()
        return carry

    lax.fori_loop(1, devices, take_piece, 0)

    for b in range(nb):
        wide = shapes_wide[b]
        whole = jnp.concatenate([table[g, b] for g in range(ng)], axis=1)
        half = jnp.dot(wide, whole, precision=HIGH, preferred_element_type=jnp.float32)
        full = lax.dot_general(half, wide, NT, precision=HIGH, preferred_element_type=jnp.float32)
        turned = full.T
        even = (0.5 * (full + turned))[0:modes]
        odd = (0.5 * (full - turned))[0:modes]

        def numer_block(blk, carry):
            first = pl.multiple_of(blk * BLOCK, BLOCK)
            for k in range(BLOCK):
                put(k, even * u_scr[b, first + k] - odd * v_scr[b, first + k])
            score = forms(b) / (denom[b, pl.ds(first, BLOCK), :] * float(bins))
            for g in range(ng):
                for s in range(BLOCK // share):
                    value = score[s * share : (s + 1) * share, g * depth_here : (g + 1) * depth_here]
                    slot = blk * (BLOCK // share) + s
                    if b == 0:
                        power[g, slot] = value
                    else:
                        power[g, slot] += value
            return carry

        lax.fori_loop(0, ranges // BLOCK, numer_block, 0)

    def part(k):
        peer = lax.rem(me + k, devices)
        peer_f, peer_g = peer // ng, lax.rem(peer, ng)
        return pltpu.make_async_remote_copy(
            src_ref=power.at[peer_g, peer_f],
            dst_ref=parts.at[k],
            send_sem=part_send.at[k],
            recv_sem=part_recv.at[k],
            device_id=(peer_f, peer_g),
            device_id_type=MESH,
        )

    def send_part(k, carry):
        part(k).start()
        return carry

    lax.fori_loop(1, devices, send_part, 0)
    parts[0] = power[my_g, my_f]

    def finish(k, carry):
        piece(k).wait_send()
        part(k).wait()
        return carry

    for k in range(1, ng):
        for copy in mode_copies(k):
            copy.wait_send()
    lax.fori_loop(1, devices, finish, 0)
    out_ref[...] = jnp.sum(parts[...], axis=0)


def solution(mesh):
    nf, ng = mesh.shape["freq"], mesh.shape["grid"]
    devices = nf * ng

    def per_device(cross_spectra, sensor_modes, source_modes, wavenumber, attenuation, mode_counts):
        two, bins, rows, cols = cross_spectra.shape
        bins_here, modes, _ = sensor_modes.shape
        depth_here = source_modes.shape[2]
        nb = bins_here // ng
        ranges = RANGES // nf * nf
        share = ranges // nf
        f32, bf16 = jnp.float32, jnp.bfloat16
        dma = pltpu.SemaphoreType.DMA
        return pl.pallas_call(
            functools.partial(kernel, nf, ng),
            out_shape=jax.ShapeDtypeStruct((share, depth_here), f32),
            in_specs=[pl.BlockSpec(memory_space=pl.ANY)] * 3
            + [pl.BlockSpec(memory_space=pltpu.VMEM)] * 2
            + [pl.BlockSpec(memory_space=pltpu.SMEM)],
            out_specs=pl.BlockSpec(memory_space=pltpu.VMEM),
            scratch_shapes=[
                pltpu.VMEM((two, bins, rows, cols), f32),
                pltpu.VMEM((bins, rows, cols), f32),
                pltpu.VMEM((ng, nb, nf * rows, cols), f32),
                pltpu.VMEM((ng, nb, modes, cols), f32),
                pltpu.VMEM((ng, nb, modes, depth_here), f32),
                pltpu.VMEM((nb, LANES, ng * cols), f32),
                pltpu.VMEM((nb, 2 * LANES, ng * depth_here), bf16),
                pltpu.VMEM((nb, modes, ng * depth_here), f32),
                pltpu.VMEM((nb, 2, ranges, LANES), f32),
                pltpu.VMEM((nb, 2, ranges // BLOCK, modes, BLOCK), f32),
                pltpu.VMEM((8, LANES), f32),
                pltpu.VMEM((nb, ranges, modes, LANES), f32),
                pltpu.VMEM((nb, ranges, modes, LANES), f32),
                pltpu.VMEM((BLOCK * modes, 2 * LANES), bf16),
                pltpu.VMEM((nb, ranges, ng * depth_here), f32),
                pltpu.VMEM((ng, nf, share, depth_here), f32),
                pltpu.VMEM((devices, share, depth_here), f32),
                dma, dma((2,)), dma((2, ng)), dma((2, ng)),
                dma((devices,)), dma((devices,)), dma((devices,)), dma((devices,)),
            ],
            compiler_params=pltpu.CompilerParams(
                collective_id=0, has_side_effects=True, vmem_limit_bytes=60 * 1024 * 1024
            ),
        )(cross_spectra, sensor_modes, source_modes, wavenumber, attenuation, mode_counts)

    placed = (
        P(None, None, "freq", "grid"),
        P("freq", None, "grid"),
        P("freq", None, "grid"),
        P("freq", None),
        P("freq", None),
        P("freq"),
    )
    return jax.shard_map(
        per_device, mesh=mesh, in_specs=placed, out_specs=P("freq", "grid"), check_vma=False
    )
```

```python
import functools

import jax
import jax.numpy as jnp
from jax import lax
from jax.experimental import pallas as pl
from jax.experimental.pallas import tpu as pltpu
from jax.sharding import PartitionSpec as P

RANGES = 64
BLOCK = 8
STEP = 2
LANES = 128

HIGH = lax.Precision.HIGHEST
MESH = pl.DeviceIdType.MESH
NT = (((1,), (1,)), ((), ()))


def kernel(
    nf, ng,
    spectra_hbm, sensor_hbm, source_hbm, wave_ref, atten_ref, counts_ref,
    out_ref,
    raw, outgoing, table, shapes, sources, shapes_wide, halves, weight, rows_scr, cols_scr, row_in,
    u_scr, v_scr, lhs, denom, power, parts,
    raw_sem, own_sem, mode_send, mode_recv, send_sem, recv_sem, part_send, part_recv,
):
    devices = nf * ng
    bins = outgoing.shape[0]
    nb = bins // devices
    row_count, col_count = raw.shape[2], raw.shape[3]
    modes = shapes.shape[2]
    ranges = u_scr.shape[1]
    share = ranges // nf
    depth_here = sources.shape[3]
    my_f, my_g = lax.axis_index("freq"), lax.axis_index("grid")
    me = my_f * ng + my_g

    raw_copy = pltpu.make_async_copy(spectra_hbm, raw, raw_sem)
    raw_copy.start()
    own = pl.ds(my_g * nb, nb)
    own_shapes = pltpu.make_async_copy(sensor_hbm.at[own], shapes.at[my_g], own_sem.at[0])
    own_sources = pltpu.make_async_copy(source_hbm.at[own], sources.at[my_g], own_sem.at[1])
    own_shapes.start()
    own_sources.start()

    barrier = pltpu.get_barrier_semaphore()

    def greet(k, carry):
        peer = lax.rem(me + k, devices)
        pl.semaphore_signal(
            barrier, inc=1, device_id=(peer // ng, lax.rem(peer, ng)), device_id_type=MESH
        )
        return carry

    lax.fori_loop(1, devices, greet, 0)

    raw_copy.wait()
    outgoing[...] = raw[0] + raw[1]
    my_rows = pl.ds(pl.multiple_of(my_f * row_count, row_count), row_count)
    for b in range(nb):
        table[my_g, b, my_rows, :] = outgoing[me * nb + b]

    pl.semaphore_wait(barrier, devices - 1)

    def mode_copies(k):
        peer = lax.rem(my_g + k, ng)
        theirs = pl.ds(peer * nb, nb)
        return [
            pltpu.make_async_remote_copy(
                src_ref=hbm.at[theirs],
                dst_ref=here.at[my_g],
                send_sem=mode_send.at[i, k],
                recv_sem=mode_recv.at[i, k],
                device_id=(my_f, peer),
                device_id_type=MESH,
            )
            for i, (hbm, here) in enumerate(((sensor_hbm, shapes), (source_hbm, sources)))
        ]

    for k in range(1, ng):
        for copy in mode_copies(k):
            copy.start()

    def piece(k):
        peer = lax.rem(me + k, devices)
        return pltpu.make_async_remote_copy(
            src_ref=outgoing.at[pl.ds(peer * nb, nb)],
            dst_ref=table.at[my_g, :, my_rows, :],
            send_sem=send_sem.at[k],
            recv_sem=recv_sem.at[k],
            device_id=(peer // ng, lax.rem(peer, ng)),
            device_id_type=MESH,
        )

    def send_piece(k, carry):
        piece(k).start()
        return carry

    lax.fori_loop(1, devices, lambda k, c: send_piece(devices - k, c), 0)

    for b in range(nb):
        row = my_g * nb + b
        row_in[...] = jnp.ones_like(row_in)
        row_in[0:1, 0:modes] = wave_ref[pl.ds(row, 1), :]
        row_in[1:2, 0:modes] = atten_ref[pl.ds(row, 1), :]
        radius = 1.0 + lax.broadcasted_iota(jnp.int32, (ranges, LANES), 0).astype(jnp.float32)
        lane = lax.broadcasted_iota(jnp.int32, (ranges, LANES), 1)
        phase = radius * row_in[0:1, :]
        magnitude = jnp.exp(-row_in[1:2, :] * radius) / jnp.sqrt(phase)
        magnitude = jnp.where(lane < counts_ref[row], magnitude, 0.0)
        filler = jnp.zeros((LANES - ranges, LANES), jnp.float32)
        for i, factor in enumerate((magnitude * jnp.cos(phase), magnitude * jnp.sin(phase))):
            rows_scr[b, i] = factor
            turned = jnp.concatenate([factor, filler], 0).T
            for blk in range(ranges // BLOCK):
                cols_scr[b, i, blk] = turned[0:modes, blk * BLOCK : (blk + 1) * BLOCK]

    for b in range(nb):

        def pair_block(blk, carry):
            first = pl.multiple_of(blk * BLOCK, BLOCK)
            row_real = rows_scr[b, 0, pl.ds(first, BLOCK), :]
            row_imag = rows_scr[b, 1, pl.ds(first, BLOCK), :]
            col_real, col_imag = cols_scr[b, 0, blk], cols_scr[b, 1, blk]
            for k in range(BLOCK):
                nr, ni = row_real[k : k + 1, :], row_imag[k : k + 1, :]
                mr = jnp.broadcast_to(col_real[:, k : k + 1], (modes, LANES))
                mi = jnp.broadcast_to(col_imag[:, k : k + 1], (modes, LANES))
                u_scr[b, first + k] = mr * nr + mi * ni
                v_scr[b, first + k] = mr * ni - mi * nr
            return carry

        lax.fori_loop(0, ranges // BLOCK, pair_block, 0)

    own_shapes.wait()
    own_sources.wait()
    for k in range(1, ng):
        for copy in mode_copies(k):
            copy.wait_recv()

    shapes_wide[...] = jnp.zeros_like(shapes_wide)
    halves[...] = jnp.zeros_like(halves)
    for b in range(nb):
        for g in range(ng):
            shapes_wide[b, 0:modes, g * col_count : (g + 1) * col_count] = shapes[g, b]
            exact = sources[g, b]
            rounded = exact.astype(jnp.bfloat16)
            at = slice(g * depth_here, (g + 1) * depth_here)
            halves[b, 0:modes, at] = rounded
            halves[b, LANES : LANES + modes, at] = rounded
            weight[b, :, at] = 2.0 * exact - rounded.astype(jnp.float32)

    def put(i, k, block):
        high = block.astype(jnp.bfloat16)
        low = (block - high.astype(jnp.float32)).astype(jnp.bfloat16)
        lhs[i, k * modes : (k + 1) * modes, 0:LANES] = high
        lhs[i, k * modes : (k + 1) * modes, LANES : 2 * LANES] = low

    def forms(i, b):
        image = jnp.dot(lhs[i], halves[b], preferred_element_type=jnp.float32)
        image = image.reshape(BLOCK, modes, image.shape[1]) * weight[b][None]
        return jnp.sum(image, axis=1)

    for b in range(nb):
        wide = shapes_wide[b]
        gram = lax.dot_general(
            wide[0:modes], wide, NT, precision=HIGH, preferred_element_type=jnp.float32
        )

        def denom_step(step, carry):
            for i in range(STEP):
                first = pl.multiple_of((step * STEP + i) * BLOCK, BLOCK)
                for k in range(BLOCK):
                    put(i, k, gram * u_scr[b, first + k])
                denom[b, pl.ds(first, BLOCK), :] = forms(i, b) * float(bins)
            return carry

        lax.fori_loop(0, ranges // BLOCK // STEP, denom_step, 0)

    def take_piece(k, carry):
        piece(k).wait_recv()
        return carry

    lax.fori_loop(1, devices, take_piece, 0)

    for b in range(nb):
        wide = shapes_wide[b]
        whole = jnp.concatenate([table[g, b] for g in range(ng)], axis=1)
        half = jnp.dot(wide, whole, precision=HIGH, preferred_element_type=jnp.float32)
        full = lax.dot_general(half, wide, NT, precision=HIGH, preferred_element_type=jnp.float32)
        turned = full.T
        even = (0.5 * (full + turned))[0:modes]
        odd = (0.5 * (full - turned))[0:modes]

        def numer_step(step, carry):
            for i in range(STEP):
                blk = step * STEP + i
                first = pl.multiple_of(blk * BLOCK, BLOCK)
                for k in range(BLOCK):
                    put(i, k, even * u_scr[b, first + k] - odd * v_scr[b, first + k])
                score = forms(i, b) / denom[b, pl.ds(first, BLOCK), :]
                for g in range(ng):
                    for t in range(BLOCK // share):
                        at = slice(g * depth_here, (g + 1) * depth_here)
                        value = score[t * share : (t + 1) * share, at]
                        slot = blk * (BLOCK // share) + t
                        if b == 0:
                            power[g, slot] = value
                        else:
                            power[g, slot] += value
            return carry

        lax.fori_loop(0, ranges // BLOCK // STEP, numer_step, 0)

    def part(k):
        peer = lax.rem(me + k, devices)
        peer_f, peer_g = peer // ng, lax.rem(peer, ng)
        return pltpu.make_async_remote_copy(
            src_ref=power.at[peer_g, peer_f],
            dst_ref=parts.at[k],
            send_sem=part_send.at[k],
            recv_sem=part_recv.at[k],
            device_id=(peer_f, peer_g),
            device_id_type=MESH,
        )

    def send_part(k, carry):
        part(k).start()
        return carry

    lax.fori_loop(1, devices, send_part, 0)
    parts[0] = power[my_g, my_f]

    def finish(k, carry):
        piece(k).wait_send()
        part(k).wait()
        return carry

    for k in range(1, ng):
        for copy in mode_copies(k):
            copy.wait_send()
    lax.fori_loop(1, devices, finish, 0)
    out_ref[...] = jnp.sum(parts[...], axis=0)


def solution(mesh):
    nf, ng = mesh.shape["freq"], mesh.shape["grid"]
    devices = nf * ng

    def per_device(cross_spectra, sensor_modes, source_modes, wavenumber, attenuation, mode_counts):
        two, bins, rows, cols = cross_spectra.shape
        bins_here, modes, _ = sensor_modes.shape
        depth_here = source_modes.shape[2]
        nb = bins_here // ng
        ranges = RANGES // nf * nf
        share = ranges // nf
        f32, bf16 = jnp.float32, jnp.bfloat16
        dma = pltpu.SemaphoreType.DMA
        return pl.pallas_call(
            functools.partial(kernel, nf, ng),
            out_shape=jax.ShapeDtypeStruct((share, depth_here), f32),
            in_specs=[pl.BlockSpec(memory_space=pl.ANY)] * 3
            + [pl.BlockSpec(memory_space=pltpu.VMEM)] * 2
            + [pl.BlockSpec(memory_space=pltpu.SMEM)],
            out_specs=pl.BlockSpec(memory_space=pltpu.VMEM),
            scratch_shapes=[
                pltpu.VMEM((two, bins, rows, cols), f32),
                pltpu.VMEM((bins, rows, cols), f32),
                pltpu.VMEM((ng, nb, nf * rows, cols), f32),
                pltpu.VMEM((ng, nb, modes, cols), f32),
                pltpu.VMEM((ng, nb, modes, depth_here), f32),
                pltpu.VMEM((nb, LANES, ng * cols), f32),
                pltpu.VMEM((nb, 2 * LANES, ng * depth_here), bf16),
                pltpu.VMEM((nb, modes, ng * depth_here), f32),
                pltpu.VMEM((nb, 2, ranges, LANES), f32),
                pltpu.VMEM((nb, 2, ranges // BLOCK, modes, BLOCK), f32),
                pltpu.VMEM((8, LANES), f32),
                pltpu.VMEM((nb, ranges, modes, LANES), f32),
                pltpu.VMEM((nb, ranges, modes, LANES), f32),
                pltpu.VMEM((STEP, BLOCK * modes, 2 * LANES), bf16),
                pltpu.VMEM((nb, ranges, ng * depth_here), f32),
                pltpu.VMEM((ng, nf, share, depth_here), f32),
                pltpu.VMEM((devices, share, depth_here), f32),
                dma, dma((2,)), dma((2, ng)), dma((2, ng)),
                dma((devices,)), dma((devices,)), dma((devices,)), dma((devices,)),
            ],
            compiler_params=pltpu.CompilerParams(
                collective_id=0, has_side_effects=True, vmem_limit_bytes=60 * 1024 * 1024
            ),
        )(cross_spectra, sensor_modes, source_modes, wavenumber, attenuation, mode_counts)

    placed = (
        P(None, None, "freq", "grid"),
        P("freq", None, "grid"),
        P("freq", None, "grid"),
        P("freq", None),
        P("freq", None),
        P("freq"),
    )
    return jax.shard_map(
        per_device, mesh=mesh, in_specs=placed, out_specs=P("freq", "grid"), check_vma=False
    )
```

```python
import functools

import jax
import jax.numpy as jnp
from jax import lax
from jax.experimental import pallas as pl
from jax.experimental.pallas import tpu as pltpu
from jax.sharding import PartitionSpec as P

RANGES = 64
BLOCK = 8
STEP = 8
LANES = 128

HIGH = lax.Precision.HIGHEST
MESH = pl.DeviceIdType.MESH
NT = (((1,), (1,)), ((), ()))
NN = (((1,), (0,)), ((), ()))


def split(value):
    high = value.astype(jnp.bfloat16)
    return high, (value - high.astype(jnp.float32)).astype(jnp.bfloat16)


def product(left, right, dims):
    return lax.dot_general(left, right, dims, preferred_element_type=jnp.float32)


def kernel(
    nf, ng,
    spectra_hbm, sensor_hbm, source_hbm, wave_ref, atten_ref, counts_ref,
    out_ref,
    raw, outgoing, table, shapes, sources, shapes_wide, halves, weight, rows_scr, cols_scr, row_in,
    u_scr, v_scr, lhs, denom, power, parts,
    raw_sem, own_sem, mode_send, mode_recv, send_sem, recv_sem, part_send, part_recv,
):
    devices = nf * ng
    bins = outgoing.shape[0]
    nb = bins // devices
    row_count, col_count = raw.shape[2], raw.shape[3]
    modes = shapes.shape[2]
    ranges = u_scr.shape[1]
    share = ranges // nf
    depth_here = sources.shape[3]
    my_f, my_g = lax.axis_index("freq"), lax.axis_index("grid")
    me = my_f * ng + my_g

    raw_copy = pltpu.make_async_copy(spectra_hbm, raw, raw_sem)
    raw_copy.start()
    own = pl.ds(my_g * nb, nb)
    own_shapes = pltpu.make_async_copy(sensor_hbm.at[own], shapes.at[my_g], own_sem.at[0])
    own_sources = pltpu.make_async_copy(source_hbm.at[own], sources.at[my_g], own_sem.at[1])
    own_shapes.start()
    own_sources.start()

    barrier = pltpu.get_barrier_semaphore()

    def greet(k, carry):
        peer = lax.rem(me + k, devices)
        pl.semaphore_signal(
            barrier, inc=1, device_id=(peer // ng, lax.rem(peer, ng)), device_id_type=MESH
        )
        return carry

    lax.fori_loop(1, devices, greet, 0)

    raw_copy.wait()
    outgoing[...] = raw[0] + raw[1]
    my_rows = pl.ds(pl.multiple_of(my_f * row_count, row_count), row_count)
    for b in range(nb):
        table[my_g, b, my_rows, :] = outgoing[me * nb + b]

    pl.semaphore_wait(barrier, devices - 1)

    def mode_copies(k):
        peer = lax.rem(my_g + k, ng)
        theirs = pl.ds(peer * nb, nb)
        return [
            pltpu.make_async_remote_copy(
                src_ref=hbm.at[theirs],
                dst_ref=here.at[my_g],
                send_sem=mode_send.at[i, k],
                recv_sem=mode_recv.at[i, k],
                device_id=(my_f, peer),
                device_id_type=MESH,
            )
            for i, (hbm, here) in enumerate(((sensor_hbm, shapes), (source_hbm, sources)))
        ]

    for k in range(1, ng):
        for copy in mode_copies(k):
            copy.start()

    def piece(k):
        peer = lax.rem(me + k, devices)
        return pltpu.make_async_remote_copy(
            src_ref=outgoing.at[pl.ds(peer * nb, nb)],
            dst_ref=table.at[my_g, :, my_rows, :],
            send_sem=send_sem.at[k],
            recv_sem=recv_sem.at[k],
            device_id=(peer // ng, lax.rem(peer, ng)),
            device_id_type=MESH,
        )

    def send_piece(k, carry):
        piece(k).start()
        return carry

    lax.fori_loop(1, devices, lambda k, c: send_piece(devices - k, c), 0)

    for b in range(nb):
        row = my_g * nb + b
        row_in[...] = jnp.ones_like(row_in)
        row_in[0:1, 0:modes] = wave_ref[pl.ds(row, 1), :]
        row_in[1:2, 0:modes] = atten_ref[pl.ds(row, 1), :]
        radius = 1.0 + lax.broadcasted_iota(jnp.int32, (ranges, LANES), 0).astype(jnp.float32)
        lane = lax.broadcasted_iota(jnp.int32, (ranges, LANES), 1)
        phase = radius * row_in[0:1, :]
        magnitude = jnp.exp(-row_in[1:2, :] * radius) / jnp.sqrt(phase)
        magnitude = jnp.where(lane < counts_ref[row], magnitude, 0.0)
        filler = jnp.zeros((LANES - ranges, LANES), jnp.float32)
        for i, factor in enumerate((magnitude * jnp.cos(phase), magnitude * jnp.sin(phase))):
            rows_scr[b, i] = factor
            turned = jnp.concatenate([factor, filler], 0).T
            for blk in range(ranges // BLOCK):
                cols_scr[b, i, blk] = turned[0:modes, blk * BLOCK : (blk + 1) * BLOCK]

    for b in range(nb):

        def pair_block(blk, carry):
            first = pl.multiple_of(blk * BLOCK, BLOCK)
            row_real = rows_scr[b, 0, pl.ds(first, BLOCK), :]
            row_imag = rows_scr[b, 1, pl.ds(first, BLOCK), :]
            col_real, col_imag = cols_scr[b, 0, blk], cols_scr[b, 1, blk]
            for k in range(BLOCK):
                nr, ni = row_real[k : k + 1, :], row_imag[k : k + 1, :]
                mr = jnp.broadcast_to(col_real[:, k : k + 1], (modes, LANES))
                mi = jnp.broadcast_to(col_imag[:, k : k + 1], (modes, LANES))
                u_scr[b, first + k] = mr * nr + mi * ni
                v_scr[b, first + k] = mr * ni - mi * nr
            return carry

        lax.fori_loop(0, ranges // BLOCK, pair_block, 0)

    own_shapes.wait()
    own_sources.wait()
    for k in range(1, ng):
        for copy in mode_copies(k):
            copy.wait_recv()

    shapes_wide[...] = jnp.zeros_like(shapes_wide)
    halves[...] = jnp.zeros_like(halves)
    for b in range(nb):
        for g in range(ng):
            shapes_wide[b, 0:modes, g * col_count : (g + 1) * col_count] = shapes[g, b]
            exact = sources[g, b]
            rounded = exact.astype(jnp.bfloat16)
            at = slice(g * depth_here, (g + 1) * depth_here)
            halves[b, 0:modes, at] = rounded
            halves[b, LANES : LANES + modes, at] = rounded
            weight[b, :, at] = 2.0 * exact - rounded.astype(jnp.float32)

    def put(i, k, block):
        high = block.astype(jnp.bfloat16)
        low = (block - high.astype(jnp.float32)).astype(jnp.bfloat16)
        lhs[i, k * modes : (k + 1) * modes, 0:LANES] = high
        lhs[i, k * modes : (k + 1) * modes, LANES : 2 * LANES] = low

    def forms(i, b):
        image = jnp.dot(lhs[i], halves[b], preferred_element_type=jnp.float32)
        image = image.reshape(BLOCK, modes, image.shape[1]) * weight[b][None]
        return jnp.sum(image, axis=1)

    for b in range(nb):
        wide = shapes_wide[b]
        gram = lax.dot_general(
            wide[0:modes], wide, NT, precision=HIGH, preferred_element_type=jnp.float32
        )

        def denom_step(step, carry):
            for i in range(STEP):
                first = pl.multiple_of((step * STEP + i) * BLOCK, BLOCK)
                for k in range(BLOCK):
                    put(i, k, gram * u_scr[b, first + k])
                denom[b, pl.ds(first, BLOCK), :] = forms(i, b) * float(bins)
            return carry

        lax.fori_loop(0, ranges // BLOCK // STEP, denom_step, 0)

    def part(peer, slot):
        peer_f, peer_g = peer // ng, lax.rem(peer, ng)
        return pltpu.make_async_remote_copy(
            src_ref=power.at[peer_g, peer_f],
            dst_ref=parts.at[slot],
            send_sem=part_send.at[peer],
            recv_sem=part_recv.at[slot],
            device_id=(peer_f, peer_g),
            device_id_type=MESH,
        )

    blocks = ranges // BLOCK
    owners = BLOCK // share
    low = 1 - (my_f // owners * 2) // blocks

    def block_at(n):
        return lax.rem(my_f // owners + (1 - 2 * low) * (n + 1) + blocks, blocks)

    def send_block(n):
        for t in range(owners):
            for g in range(ng):
                part((block_at(n) * owners + t) * ng + g, me).start()

    def take_piece(k, carry):
        piece(k).wait_recv()
        return carry

    lax.fori_loop(1, devices, take_piece, 0)

    for b in range(nb):
        wide = shapes_wide[b]
        whole = jnp.concatenate([table[g, b] for g in range(ng)], axis=1)
        left_high, left_low = split(wide)
        mid_high, mid_low = split(whole)
        both = jnp.concatenate([left_high, left_low], 0)
        half = product(both, mid_high, NN)
        half = half[:LANES] + (half[LANES:] + product(left_high, mid_low, NN))
        half_high, half_low = split(half)
        both = jnp.concatenate([half_high, half_low], 0)
        full = product(both, left_high, NT)
        full = full[:LANES] + (full[LANES:] + product(half_high, left_low, NT))
        turned = full.T
        even = (0.5 * (full + turned))[0:modes]
        odd = (0.5 * (full - turned))[0:modes]

        def numer_step(step, carry):
            for i in range(STEP):
                blk = block_at(step * STEP + i)
                first = pl.multiple_of(blk * BLOCK, BLOCK)
                for k in range(BLOCK):
                    put(i, k, even * u_scr[b, first + k] - odd * v_scr[b, first + k])
                score = forms(i, b) / denom[b, pl.ds(first, BLOCK), :]
                for g in range(ng):
                    for t in range(owners):
                        at = slice(g * depth_here, (g + 1) * depth_here)
                        value = score[t * share : (t + 1) * share, at]
                        slot = blk * owners + t
                        if b == 0:
                            power[g, slot] = value
                        else:
                            power[g, slot] += value
                if b == nb - 1 and i > 0:
                    send_block(step * STEP + i - 1)
                elif b == nb - 1:

                    @pl.when(step > 0)
                    def _():
                        send_block(step * STEP - 1)

            return carry

        lax.fori_loop(0, ranges // BLOCK // STEP, numer_step, 0)

    def send_last(k, carry):
        peer = me // (owners * ng) * (owners * ng) + lax.rem(me + k, owners * ng)
        part(peer, me).start()
        return carry

    lax.fori_loop(1, owners * ng, send_last, 0)
    parts[me] = power[my_g, my_f]

    def finish(k, carry):
        piece(k).wait_send()
        peer = lax.rem(me + k, devices)
        part(peer, me).wait_send()
        part(peer, peer).wait_recv()
        return carry

    for k in range(1, ng):
        for copy in mode_copies(k):
            copy.wait_send()
    lax.fori_loop(1, devices, finish, 0)
    out_ref[...] = jnp.sum(parts[...], axis=0)


def solution(mesh):
    nf, ng = mesh.shape["freq"], mesh.shape["grid"]
    devices = nf * ng

    def per_device(cross_spectra, sensor_modes, source_modes, wavenumber, attenuation, mode_counts):
        two, bins, rows, cols = cross_spectra.shape
        bins_here, modes, _ = sensor_modes.shape
        depth_here = source_modes.shape[2]
        nb = bins_here // ng
        ranges = RANGES // nf * nf
        share = ranges // nf
        f32, bf16 = jnp.float32, jnp.bfloat16
        dma = pltpu.SemaphoreType.DMA
        return pl.pallas_call(
            functools.partial(kernel, nf, ng),
            out_shape=jax.ShapeDtypeStruct((share, depth_here), f32),
            in_specs=[pl.BlockSpec(memory_space=pl.ANY)] * 3
            + [pl.BlockSpec(memory_space=pltpu.VMEM)] * 2
            + [pl.BlockSpec(memory_space=pltpu.SMEM)],
            out_specs=pl.BlockSpec(memory_space=pltpu.VMEM),
            scratch_shapes=[
                pltpu.VMEM((two, bins, rows, cols), f32),
                pltpu.VMEM((bins, rows, cols), f32),
                pltpu.VMEM((ng, nb, nf * rows, cols), f32),
                pltpu.VMEM((ng, nb, modes, cols), f32),
                pltpu.VMEM((ng, nb, modes, depth_here), f32),
                pltpu.VMEM((nb, LANES, ng * cols), f32),
                pltpu.VMEM((nb, 2 * LANES, ng * depth_here), bf16),
                pltpu.VMEM((nb, modes, ng * depth_here), f32),
                pltpu.VMEM((nb, 2, ranges, LANES), f32),
                pltpu.VMEM((nb, 2, ranges // BLOCK, modes, BLOCK), f32),
                pltpu.VMEM((8, LANES), f32),
                pltpu.VMEM((nb, ranges, modes, LANES), f32),
                pltpu.VMEM((nb, ranges, modes, LANES), f32),
                pltpu.VMEM((STEP, BLOCK * modes, 2 * LANES), bf16),
                pltpu.VMEM((nb, ranges, ng * depth_here), f32),
                pltpu.VMEM((ng, nf, share, depth_here), f32),
                pltpu.VMEM((devices, share, depth_here), f32),
                dma, dma((2,)), dma((2, ng)), dma((2, ng)),
                dma((devices,)), dma((devices,)), dma((devices,)), dma((devices,)),
            ],
            compiler_params=pltpu.CompilerParams(
                collective_id=0, has_side_effects=True, vmem_limit_bytes=60 * 1024 * 1024
            ),
        )(cross_spectra, sensor_modes, source_modes, wavenumber, attenuation, mode_counts)

    placed = (
        P(None, None, "freq", "grid"),
        P("freq", None, "grid"),
        P("freq", None, "grid"),
        P("freq", None),
        P("freq", None),
        P("freq"),
    )
    return jax.shard_map(
        per_device, mesh=mesh, in_specs=placed, out_specs=P("freq", "grid"), check_vma=False
    )
```
